32 devices in a mesh: samp: 8 (over z, x), win: 1, snp: 4 (over y, core).
Axes of the slice: x: 2, y: 2, z: 4, core: 2. Of those that a mesh axis runs over, the one named last changes fastest.
Arguments:
- dosages: bfloat16 [4096, 4096], P('samp', ('win', 'snp')), may hold values from 0 to 2
Outputs:
- r_squared: float32 [1, 4096, 4096], P('win', 'samp', 'snp')
- band_r_squared: float32 [1, 1024, 4096], P('win', 'samp', 'snp')
The draws below stay inside these ranges and needn't reach their ends.
All inputs are finite; a program needn't handle non-finite values.
Results may differ from the reference program's by a relative error of at most 0.0003.
Values may be sent and summed in bfloat16 or wider, within the bound.
No kernel may reach another device: no remote copies, remote signals or barrier semaphores. Data moves between devices by JAX's collectives and lax.ppermute only.
A program may use at most 128 MiB of HBM per device.

```python
import jax
import jax.numpy as jnp
from jax import lax

WS = 4096
OV = 1024
WINDOWS = 1
SAMPLES = 4096
SNPS = 4096


def draw_dosages(key, part):
    keys = jax.random.split(key, 5)
    span = min(24, SNPS)
    noise = jax.random.normal(keys[0], (SAMPLES, SNPS), jnp.float32)
    smooth = lax.reduce_window(noise, 0.0, lax.add, (1, span), (1, 1), 'SAME') / span ** 0.5
    own_weight = jax.random.uniform(keys[1], (SNPS,), jnp.float32, 0.3, 1.0)
    mix_weight = jax.random.uniform(keys[2], (SNPS,), jnp.float32, 0.5, 2.5)
    people = jax.random.normal(keys[3], (SAMPLES, 1), jnp.float32)
    loading = jax.random.normal(keys[4], (SNPS,), jnp.float32) * 0.6
    latent = noise * own_weight + smooth * mix_weight
    latent = latent + people * loading
    return (2.0 * jax.nn.sigmoid(latent)).astype(jnp.bfloat16)


def setup_inputs(seed: int = 0) -> dict:
    seeds = jax.random.split(jax.random.key(seed), 2)
    return {
        "dosages": draw_dosages(jax.random.fold_in(seeds[1], 71), 0),
    }


var_floor = 0.05


def squared_corr(gram, col_sum, col_sq, row_sum, row_sq, count):
    col_mean = col_sum / count
    row_mean = row_sum / count
    col_var = jnp.maximum(col_sq / count - col_mean * col_mean, var_floor)
    row_var = jnp.maximum(row_sq / count - row_mean * row_mean, var_floor)
    covar = gram / count - col_mean[:, None] * row_mean[None, :]
    return covar * covar / (col_var[:, None] * row_var[None, :])


def column_stats(block):
    wide = block.astype(jnp.float32)
    return jnp.sum(wide, axis=0), jnp.sum(wide * wide, axis=0)


def reference(dosages):
    count = jnp.float32(dosages.shape[0])
    whole_list = []
    band_list = []
    for window in range(WINDOWS):
        geno = dosages[:, window * WS:(window + 1) * WS]
        following = (window + 1) % WINDOWS
        after = dosages[:, following * WS:following * WS + OV]
        win_sum, win_sq = column_stats(geno)
        next_sum, next_sq = column_stats(after)
        gram = jnp.dot(geno.T, geno, preferred_element_type=jnp.float32)
        next_gram = jnp.dot(after.T, geno, preferred_element_type=jnp.float32)
        whole_list.append(squared_corr(gram, win_sum, win_sq, win_sum, win_sq, count))
        band_list.append(squared_corr(next_gram, next_sum, next_sq, win_sum, win_sq, count))
    return jnp.stack(whole_list), jnp.stack(band_list)
```

```python
import functools

import jax
import jax.numpy as jnp
from jax import lax
from jax.experimental import pallas as pl
from jax.experimental.pallas import tpu as pltpu
from jax.sharding import PartitionSpec as P


OV = 1024


var_floor = 0.05


def ring_pairs(size, step):
    order = list(range(0, size, 2)) + list(range(1, size, 2))[::-1]
    return [(order[i], order[(i + step) % size]) for i in range(size)]


def ring_chunks(own):
    size = lax.axis_size("samp")
    half = own.shape[0] // 2
    ahead = ring_pairs(size, 1)
    back = ring_pairs(size, -1)
    fore = [own[:half], own[half:]]
    aft = [own[half:], own[:half]]
    groups = [[own[:half], own[half:]]]
    steps = size - 1
    pending = []
    for step in range(steps):
        lane = step % 2
        fore[lane] = lax.ppermute(fore[lane], "samp", ahead)
        aft[lane] = lax.ppermute(aft[lane], "samp", back)
        pending += [fore[lane], aft[lane]]
        if lane == 1 and step < 4 or step >= 4:
            groups.append(pending)
            pending = []
    return groups


def parts_of(where, width, win_cols):
    return (
        (where[2], where[3], slice(0, win_cols)),
        (where[4], where[5], slice(win_cols, width)),
    )


def pick_columns(where, *refs, win_cols):
    out = refs[-1]
    width = out.shape[1]
    for i, chunk in enumerate(refs[:-1]):
        for at, (_, _, part) in zip((where[0], where[1]), parts_of(where, width, win_cols)):
            at = pl.ds(pl.multiple_of(at, 128), part.stop - part.start)
            out[i, part] = chunk[:, at].T


def pick_core(where, mine, theirs, out, win_cols):
    half = out.shape[0]
    base = where[6] * half
    for core, _, part in parts_of(where, out.shape[1], win_cols):

        @pl.when(core == where[6])
        def _():
            out[:, part] = mine[pl.ds(base, half), part]

        @pl.when(core != where[6])
        def _():
            out[:, part] = theirs[pl.ds(base, half), part]


def local_call(body, shape, operands, win_cols):
    vmem = pl.BlockSpec(memory_space=pltpu.VMEM)
    smem = pl.BlockSpec(memory_space=pltpu.SMEM)
    return pl.pallas_call(
        functools.partial(body, win_cols=win_cols),
        out_shape=jax.ShapeDtypeStruct(shape, jnp.bfloat16),
        in_specs=[smem] + [vmem] * (len(operands) - 1),
        out_specs=vmem,
        compiler_params=pltpu.CompilerParams(vmem_limit_bytes=8 << 20),
    )(*operands)


def wanted_rows(group, where, win_cols, band_cols):
    shape = (len(group), win_cols + band_cols, group[0].shape[0])
    mine = local_call(pick_columns, shape, (where, *group), win_cols)
    swap = [(0, 1), (1, 0), (2, 3), (3, 2)]
    across = [(0, 2), (1, 3), (2, 0), (3, 1)]
    theirs = lax.ppermute(mine, "snp", swap)
    half = (len(group) // 2,) + shape[1:]
    sent = local_call(pick_core, half, (where, mine, theirs), win_cols)
    came = lax.ppermute(sent, "snp", across)
    other = lax.ppermute(came, "snp", swap)
    return mine, theirs, came, other


def gather_rows(where, pieces, slab, win_cols):
    mine, theirs, came, other = pieces
    half = slab.shape[0] // 2
    for core, pair, part in parts_of(where, slab.shape[1], win_cols):
        near = pair == where[7]

        @pl.when(near & (core == where[6]))
        def _():
            slab[:, part] = mine[:, part]

        @pl.when(near & (core != where[6]))
        def _():
            slab[:, part] = theirs[:, part]

        @pl.when(jnp.logical_not(near) & (where[6] == 0))
        def _():
            slab[:half, part] = came[:, part]
            slab[half:, part] = other[:, part]

        @pl.when(jnp.logical_not(near) & (where[6] == 1))
        def _():
            slab[:half, part] = other[:, part]
            slab[half:, part] = came[:, part]


def add_stats(cols, slab, col_before, row_before, col_out, row_out):
    width = cols[0].shape[1]
    for out, before, op in ((0, 0, lambda v: v), (8, 8, lambda v: v * v)):
        total = None if col_before is None else col_before[before : before + 8]
        for col in cols:
            wide = op(col[...].astype(jnp.float32))
            part = jnp.sum(wide.reshape(-1, 8, width), axis=0)
            total = part if total is None else total + part
        col_out[out : out + 8] = total
    for out, op in ((0, lambda v: v), (1, lambda v: v * v)):
        total = None if row_before is None else row_before[out]
        for i in range(slab.shape[0]):
            wide = op(slab[i].astype(jnp.float32))
            for j in range(0, wide.shape[1], 128):
                part = wide[:, j : j + 128]
                total = part if total is None else total + part
        row_out[out] = total


def add_sums(cols, slab, at, before):
    total = before
    for i, col in enumerate(cols):
        part = jnp.dot(slab[i], col[:, at], preferred_element_type=jnp.float32)
        total = part if total is None else total + part
    return total


def first_sums(where, *refs, size, first, win_cols):
    cols, pieces = refs[:size], refs[size : size + 4]
    before = (None, None, None) if first else refs[size + 4 : size + 7]
    gram, col_out, row_out, slab = refs[-4:]
    gather_rows(where, pieces, slab, win_cols)
    add_stats(cols, slab, before[1], before[2], col_out, row_out)
    tile = 256

    def columns(j, carry):
        at = pl.ds(pl.multiple_of(j * tile, tile), tile)
        gram[:, at] = add_sums(cols, slab, at, None if first else before[0][:, at])
        return carry

    lax.fori_loop(0, gram.shape[1] // tile, columns, 0)


def last_sums(where, *refs, size, count, win_cols):
    cols, pieces = refs[:size], refs[size : size + 4]
    before = refs[size + 4 : size + 7]
    win_out, band_out, slab, col_stats, row_stats = refs[-5:]
    step = pl.program_id(0)

    def moments(total, square, axis):
        mean = jnp.sum(total, axis=axis, keepdims=True) / count
        square = jnp.sum(square, axis=axis, keepdims=True) / count
        return mean, 1.0 / jnp.maximum(square - mean * mean, var_floor)

    @pl.when(step == 0)
    def _():
        gather_rows(where, pieces, slab, win_cols)
        add_stats(cols, slab, before[1], before[2], col_stats, row_stats)
        mean, inverse = moments(row_stats[0], row_stats[1], 1)
        row_stats[0] = jnp.broadcast_to(mean, row_stats.shape[1:])
        row_stats[1] = jnp.broadcast_to(inverse, row_stats.shape[1:])
        mean, inverse = moments(col_stats[0:8], col_stats[8:16], 0)
        col_stats[0:1] = mean
        col_stats[1:2] = inverse

    tile = win_out.shape[1]
    at = pl.ds(pl.multiple_of(step * tile, tile), tile)
    total = add_sums(cols, slab, at, before[0][:, at])
    col_mean, col_inv = col_stats[0:1, at], col_stats[1:2, at]
    for j in range(0, tile, 128):
        part = slice(j, j + 128)
        covar = total[:, part] * (1.0 / count) - row_stats[0] * col_mean[:, part]
        ratio = covar * covar * (row_stats[1] * col_inv[:, part])
        win_out[:, part] = ratio[:win_cols]
        band_out[:, part] = ratio[win_cols:]


def summed(where, group, rows, before, last, count, win_cols):
    width = group[0].shape[1]
    row_width = rows[0].shape[1]
    operands = [where, *group, *rows] + ([] if before is None else list(before))
    gram = (row_width, width)
    sums = [gram, (16, width), (2, row_width, 128)]
    slab = pltpu.VMEM(rows[0].shape, jnp.bfloat16)
    vmem = pl.BlockSpec(memory_space=pltpu.VMEM)
    smem = pl.BlockSpec(memory_space=pltpu.SMEM)
    if last:
        tile = 256
        body = functools.partial(last_sums, size=len(group), count=count, win_cols=win_cols)
        shapes = [(win_cols, width), (row_width - win_cols, width)]
        layout = dict(
            grid=(width // tile,),
            out_specs=[pl.BlockSpec((s[0], tile), lambda j: (0, j)) for s in shapes],
            scratch_shapes=[slab] + [pltpu.VMEM(s, jnp.float32) for s in sums[1:]],
        )
    else:
        first = before is None
        body = functools.partial(first_sums, size=len(group), first=first, win_cols=win_cols)
        shapes = sums
        given = len(operands) - 3
        layout = dict(
            out_specs=[vmem] * 3,
            scratch_shapes=[slab],
            input_output_aliases={} if first else {given + i: i for i in range(3)},
        )
    return pl.pallas_call(
        body,
        out_shape=[jax.ShapeDtypeStruct(s, jnp.float32) for s in shapes],
        in_specs=[smem] + [vmem] * (len(operands) - 1),
        compiler_params=pltpu.CompilerParams(vmem_limit_bytes=16 << 20),
        **layout,
    )(*operands)


def shards(dosages):
    shard_count = lax.axis_size("samp")
    count = float(dosages.shape[0] * shard_count)
    width = dosages.shape[1]
    win_cols = width * lax.axis_size("snp") // shard_count
    band_cols = OV // shard_count
    samp, block = lax.axis_index("samp"), lax.axis_index("snp")
    row_at, band_at = samp * win_cols, samp * band_cols
    row_block, band_block = row_at // width, band_at // width
    where = jnp.stack(
        [row_at % width, band_at % width]
        + [row_block % 2, row_block // 2, band_block % 2, band_block // 2, block % 2, block // 2]
    ).astype(jnp.int32)
    groups = ring_chunks(dosages)
    rows = [wanted_rows(g, where, win_cols, band_cols) for g in groups]
    total = None
    for i, (group, row) in enumerate(zip(groups, rows)):
        last = i == len(groups) - 1
        total = summed(where, group, row, total, last, count, win_cols)
    return (total[0][None], total[1][None])


def passed_along(shard, axis, by):
    devices = lax.axis_size(axis)
    return lax.ppermute(shard, axis, [(i, (i + by) % devices) for i in range(devices)])


def squared_corr(gram, col_sum, col_sq, row_sum, row_sq, count):
    col_mean = col_sum / count
    row_mean = row_sum / count
    col_var = jnp.maximum(col_sq / count - col_mean * col_mean, var_floor)
    row_var = jnp.maximum(row_sq / count - row_mean * row_mean, var_floor)
    covar = gram / count - col_mean[:, None] * row_mean[None, :]
    return covar * covar / (col_var[:, None] * row_var[None, :])


def column_stats(block):
    return (
        jnp.sum(block, axis=0, dtype=jnp.float32),
        jnp.sum(jnp.square(block.astype(jnp.float32)), axis=0),
    )


def pair_sums(columns, own_rows):
    return lax.dot_general(
        columns, own_rows, (((0,), (0,)), ((), ())), preferred_element_type=jnp.float32
    )


def shards_by_sums(dosages):
    samples_here = dosages.shape[0]
    block_width = dosages.shape[1]
    shard_count = lax.axis_size("samp")
    count = jnp.float32(samples_here * shard_count)
    whole = lax.all_gather(dosages, "snp", axis=1, tiled=True)
    window_width = whole.shape[1]
    band = passed_along(whole[:, :OV], "win", -1)
    own_sum, own_sq = column_stats(dosages)
    total_sum, total_sq = lax.psum((own_sum, own_sq), "samp")
    win_sum, win_sq = (
        lax.all_gather(total_sum, "snp", axis=0, tiled=True),
        lax.all_gather(total_sq, "snp", axis=0, tiled=True),
    )
    next_sum, next_sq = passed_along((win_sum[:OV], win_sq[:OV]), "win", -1)
    win_cols = window_width // shard_count
    band_cols = OV // shard_count
    merged = jnp.concatenate(
        (
            whole.reshape(samples_here, shard_count, win_cols),
            band.reshape(samples_here, shard_count, band_cols),
        ),
        axis=2,
    ).reshape(samples_here, shard_count * (win_cols + band_cols))
    summed = lax.psum_scatter(pair_sums(merged, dosages), "samp", scatter_dimension=0, tiled=True)
    win_gram = summed[:win_cols]
    band_gram = summed[win_cols:]
    col_index = lax.axis_index("samp")
    row_index = lax.axis_index("snp")
    row_sum = lax.dynamic_slice_in_dim(win_sum, row_index * block_width, block_width, 0)
    row_sq = lax.dynamic_slice_in_dim(win_sq, row_index * block_width, block_width, 0)
    col_sum = lax.dynamic_slice_in_dim(win_sum, col_index * win_cols, win_cols, 0)
    col_sq = lax.dynamic_slice_in_dim(win_sq, col_index * win_cols, win_cols, 0)
    band_sum = lax.dynamic_slice_in_dim(next_sum, col_index * band_cols, band_cols, 0)
    band_sq = lax.dynamic_slice_in_dim(next_sq, col_index * band_cols, band_cols, 0)
    whole_out = squared_corr(win_gram, col_sum, col_sq, row_sum, row_sq, count)
    band_out = squared_corr(band_gram, band_sum, band_sq, row_sum, row_sq, count)
    return (whole_out[None], band_out[None])


def solution(mesh):
    near = mesh.shape["snp"] == 4 and mesh.shape["win"] == 1 and mesh.shape["samp"] == 8
    return jax.shard_map(
        shards if near else shards_by_sums,
        mesh=mesh,
        in_specs=(P("samp", ("win", "snp")),),
        out_specs=(P("win", "samp", "snp"), P("win", "samp", "snp")),
        check_vma=False,
    )
```

```python
import functools

import jax
import jax.numpy as jnp
from jax import lax
from jax.experimental import pallas as pl
from jax.experimental.pallas import tpu as pltpu
from jax.sharding import PartitionSpec as P


OV = 1024


var_floor = 0.05


def ring_pairs(size, step):
    order = list(range(0, size, 2)) + list(range(1, size, 2))[::-1]
    return [(order[i], order[(i + step) % size]) for i in range(size)]


def ring_chunks(own):
    size = lax.axis_size("samp")
    half = own.shape[0] // 2
    ahead = ring_pairs(size, 1)
    back = ring_pairs(size, -1)
    fore = [own[:half], own[half:]]
    aft = [own[half:], own[:half]]
    groups = [[own[:half], own[half:]]]
    for step in range(size - 1):
        lane = step % 2
        fore[lane] = lax.ppermute(fore[lane], "samp", ahead)
        aft[lane] = lax.ppermute(aft[lane], "samp", back)
        groups.append([fore[lane], aft[lane]])
    return groups


def parts_of(where, width, win_cols, base=0):
    return (
        (where[base + 2], where[base + 3], slice(0, win_cols)),
        (where[base + 4], where[base + 5], slice(win_cols, width)),
    )


def pick_columns(where, *refs, win_cols):
    count = (len(where) - 8) // 16
    chunks, outs = refs[: len(refs) - 1 - count], refs[len(refs) - 1 - count :]
    for i, chunk in enumerate(chunks):
        for out, base in zip(outs, (0, 8 + 8 * (i % 2))):
            parts = parts_of(where, out.shape[1], win_cols)
            for at, (_, _, part) in zip((where[base], where[base + 1]), parts):
                at = pl.ds(pl.multiple_of(at, 128), part.stop - part.start)
                out[i, part] = chunk[:, at].T


def pick_core(where, *refs, win_cols):
    outs = refs[len(refs) * 2 // 3 :]
    for i, out in enumerate(outs):
        mine, theirs = refs[2 * i : 2 * i + 2]
        half = out.shape[0]
        start = where[6] * half
        base = 0 if i == 0 else 8 + 8 * where[6]
        for core, _, part in parts_of(where, out.shape[1], win_cols, base):

            @pl.when(core == where[6])
            def _():
                out[:, part] = mine[pl.ds(start, half), part]

            @pl.when(core != where[6])
            def _():
                out[:, part] = theirs[pl.ds(start, half), part]


def local_call(body, shapes, operands, win_cols):
    vmem = pl.BlockSpec(memory_space=pltpu.VMEM)
    smem = pl.BlockSpec(memory_space=pltpu.SMEM)
    return pl.pallas_call(
        functools.partial(body, win_cols=win_cols),
        out_shape=[jax.ShapeDtypeStruct(shape, jnp.bfloat16) for shape in shapes],
        in_specs=[smem] + [vmem] * (len(operands) - 1),
        out_specs=[vmem] * len(shapes),
        compiler_params=pltpu.CompilerParams(vmem_limit_bytes=8 << 20),
    )(*operands)


def wanted_rows(groups, where, after, win_cols, band_cols):
    swap = [(0, 1), (1, 0), (2, 3), (3, 2)]
    across = [(0, 2), (1, 3), (2, 0), (3, 1)]
    size = lax.axis_size("samp")
    onward = [
        (4 * a + 2 * pair + core, 4 * b + 2 * pair + core)
        for core, step in ((0, 1), (1, -1))
        for a, b in ring_pairs(size, step)
        for pair in (0, 1)
    ]
    final = len(groups) - 1
    pieces = []
    early = None
    for index, group in enumerate(groups):
        shape = (len(group), win_cols + band_cols, group[0].shape[0])
        half = (len(group) // 2,) + shape[1:]
        ahead = index == final - 2
        at = after if ahead else where
        count = 2 if ahead else 1
        mine = local_call(pick_columns, [shape] * count, (at, *group), win_cols)
        theirs = [lax.ppermute(mine[0], "snp", swap)]
        if index == final:
            came = early
        else:
            if ahead:
                theirs.append(lax.ppermute(mine[1], "snp", swap))
            held = [piece for both in zip(mine, theirs) for piece in both]
            sent = local_call(pick_core, [half] * count, (at, *held), win_cols)
            if ahead:
                early = lax.ppermute(sent[1], "snp", across)
                early = lax.ppermute(early, ("samp", "snp"), onward)
            came = lax.ppermute(sent[0], "snp", across)
        other = lax.ppermute(came, "snp", swap)
        pieces.append((mine[0], theirs[0], came, other))
    return pieces


def gather_rows(where, pieces, slab, win_cols):
    mine, theirs, came, other = pieces
    size, row_width, rows = mine.shape

    def fill(part, places):
        for i, (piece, j) in enumerate(places):
            slab[part, i * rows : i * rows + rows] = piece[j, part]

    def pair_of(first, second):
        half = size // 2
        return [(first, j) for j in range(half)] + [(second, j) for j in range(half)]

    for core, pair, part in parts_of(where, row_width, win_cols):
        near = pair == where[7]
        far = jnp.logical_not(near)

        @pl.when(near & (core == where[6]))
        def _():
            fill(part, [(mine, j) for j in range(size)])

        @pl.when(near & (core != where[6]))
        def _():
            fill(part, [(theirs, j) for j in range(size)])

        @pl.when(far & (where[6] == 0))
        def _():
            fill(part, pair_of(came, other))

        @pl.when(far & (where[6] == 1))
        def _():
            fill(part, pair_of(other, came))


def add_stats(groups, slabs, col_before, row_before, col_out, row_out):
    for out, op in ((0, lambda v: v), (1, lambda v: v * v)):
        at = slice(8 * out, 8 * out + 8)
        total = None if col_before is None else col_before[at]
        for col in [col for cols in groups for col in cols]:
            wide = op(col[...].astype(jnp.float32))
            part = jnp.sum(wide.reshape(-1, 8, wide.shape[1]), axis=0)
            total = part if total is None else total + part
        col_out[at] = total
        total = None if row_before is None else row_before[out]
        for slab in slabs:
            for j in range(0, slab.shape[1], 128):
                part = op(slab[:, j : j + 128].astype(jnp.float32))
                total = part if total is None else total + part
        row_out[out] = total


def add_sums(groups, slabs, at, before):
    total = before
    for cols, slab in zip(groups, slabs):
        col = jnp.concatenate([col[:, at] for col in cols], axis=0)
        part = jnp.dot(slab[...], col, preferred_element_type=jnp.float32)
        total = part if total is None else total + part
    return total


def split_refs(refs, sizes):
    groups, pieces, start = [], [], 0
    for size in sizes:
        groups.append(refs[start : start + size])
        pieces.append(refs[start + size : start + size + 4])
        start += size + 4
    return groups, pieces, refs[start:]


def first_sums(where, *refs, sizes, first, win_cols):
    groups, pieces, refs = split_refs(refs, sizes)
    before = (None, None, None) if first else refs[:3]
    gram, col_out, row_out = refs[-3 - len(sizes) : -len(sizes)]
    slabs = refs[-len(sizes) :]
    for piece, slab in zip(pieces, slabs):
        gather_rows(where, piece, slab, win_cols)
    add_stats(groups, slabs, before[1], before[2], col_out, row_out)
    tile = 256

    def columns(j, carry):
        at = pl.ds(pl.multiple_of(j * tile, tile), tile)
        gram[:, at] = add_sums(groups, slabs, at, None if first else before[0][:, at])
        return carry

    lax.fori_loop(0, gram.shape[1] // tile, columns, 0)


def last_sums(where, *refs, sizes, count, win_cols):
    groups, pieces, refs = split_refs(refs, sizes)
    before, (win_out, band_out) = refs[:3], refs[3:5]
    slabs, (col_stats, row_stats) = refs[5:-2], refs[-2:]
    step = pl.program_id(0)

    def moments(total, square, axis):
        mean = jnp.sum(total, axis=axis, keepdims=True) / count
        square = jnp.sum(square, axis=axis, keepdims=True) / count
        return mean, 1.0 / jnp.maximum(square - mean * mean, var_floor)

    @pl.when(step == 0)
    def _():
        for piece, slab in zip(pieces, slabs):
            gather_rows(where, piece, slab, win_cols)
        add_stats(groups, slabs, before[1], before[2], col_stats, row_stats)
        mean, inverse = moments(row_stats[0], row_stats[1], 1)
        row_stats[0] = jnp.broadcast_to(mean, row_stats.shape[1:])
        row_stats[1] = jnp.broadcast_to(inverse, row_stats.shape[1:])
        mean, inverse = moments(col_stats[0:8], col_stats[8:16], 0)
        col_stats[0:1] = mean
        col_stats[1:2] = inverse

    tile = win_out.shape[1]
    at = pl.ds(pl.multiple_of(step * tile, tile), tile)
    total = add_sums(groups, slabs, at, before[0][:, at])
    col_mean, col_inv = col_stats[0:1, at], col_stats[1:2, at]
    for j in range(0, tile, 128):
        part = slice(j, j + 128)
        covar = total[:, part] * (1.0 / count) - row_stats[0] * col_mean[:, part]
        ratio = covar * covar * (row_stats[1] * col_inv[:, part])
        win_out[:, part] = ratio[:win_cols]
        band_out[:, part] = ratio[win_cols:]


def summed(where, groups, rows, before, last, count, win_cols):
    width = groups[0][0].shape[1]
    row_width = rows[0][0].shape[1]
    operands = [where]
    for group, row in zip(groups, rows):
        operands += [*group, *row]
    operands += [] if before is None else list(before)
    sizes = tuple(len(group) for group in groups)
    gram = (row_width, width)
    sums = [gram, (16, width), (2, row_width, 128)]
    depth = groups[0][0].shape[0]
    slabs = [pltpu.VMEM((row_width, size * depth), jnp.bfloat16) for size in sizes]
    vmem = pl.BlockSpec(memory_space=pltpu.VMEM)
    smem = pl.BlockSpec(memory_space=pltpu.SMEM)
    if last:
        tile = 512
        body = functools.partial(last_sums, sizes=sizes, count=count, win_cols=win_cols)
        shapes = [(win_cols, width), (row_width - win_cols, width)]
        layout = dict(
            grid=(width // tile,),
            out_specs=[pl.BlockSpec((s[0], tile), lambda j: (0, j)) for s in shapes],
            scratch_shapes=slabs + [pltpu.VMEM(s, jnp.float32) for s in sums[1:]],
        )
    else:
        first = before is None
        body = functools.partial(first_sums, sizes=sizes, first=first, win_cols=win_cols)
        shapes = sums
        given = len(operands) - 3
        layout = dict(
            out_specs=[vmem] * 3,
            scratch_shapes=slabs,
            input_output_aliases={} if first else {given + i: i for i in range(3)},
        )
    return pl.pallas_call(
        body,
        out_shape=[jax.ShapeDtypeStruct(s, jnp.float32) for s in shapes],
        in_specs=[smem] + [vmem] * (len(operands) - 1),
        compiler_params=pltpu.CompilerParams(vmem_limit_bytes=16 << 20),
        **layout,
    )(*operands)


def shards(dosages):
    shard_count = lax.axis_size("samp")
    count = float(dosages.shape[0] * shard_count)
    width = dosages.shape[1]
    win_cols = width * lax.axis_size("snp") // shard_count
    band_cols = OV // shard_count
    samp, block = lax.axis_index("samp"), lax.axis_index("snp")

    def place(samp):
        row_at, band_at = samp * win_cols, samp * band_cols
        row_block, band_block = row_at // width, band_at // width
        return jnp.stack(
            [row_at % width, band_at % width, row_block % 2, row_block // 2]
            + [band_block % 2, band_block // 2, block % 2, block // 2]
        ).astype(jnp.int32)

    odd, end = samp % 2 == 1, shard_count - 2
    ahead = jnp.where(odd, jnp.maximum(samp - 2, 0), jnp.where(samp == end, end + 1, samp + 2))
    back = jnp.where(odd, jnp.where(samp > end, end, samp + 2), jnp.where(samp == 0, 1, samp - 2))
    where = place(samp)
    after = jnp.concatenate((where, place(ahead), place(back)))
    groups = ring_chunks(dosages)
    *groups[0], where, after = lax.optimization_barrier((*groups[0], where, after))
    rows = wanted_rows(groups, where, after, win_cols, band_cols)
    cuts = [0, 1, 2, 3, 4, 5, len(groups) - 2, len(groups)]
    total = None
    for start, stop in zip(cuts, cuts[1:]):
        part = slice(start, stop)
        last = stop == len(groups)
        total = summed(where, groups[part], rows[part], total, last, count, win_cols)
    return (total[0][None], total[1][None])


def passed_along(shard, axis, by):
    devices = lax.axis_size(axis)
    return lax.ppermute(shard, axis, [(i, (i + by) % devices) for i in range(devices)])


def squared_corr(gram, col_sum, col_sq, row_sum, row_sq, count):
    col_mean = col_sum / count
    row_mean = row_sum / count
    col_var = jnp.maximum(col_sq / count - col_mean * col_mean, var_floor)
    row_var = jnp.maximum(row_sq / count - row_mean * row_mean, var_floor)
    covar = gram / count - col_mean[:, None] * row_mean[None, :]
    return covar * covar / (col_var[:, None] * row_var[None, :])


def column_stats(block):
    return (
        jnp.sum(block, axis=0, dtype=jnp.float32),
        jnp.sum(jnp.square(block.astype(jnp.float32)), axis=0),
    )


def pair_sums(columns, own_rows):
    return lax.dot_general(
        columns, own_rows, (((0,), (0,)), ((), ())), preferred_element_type=jnp.float32
    )


def shards_by_sums(dosages):
    samples_here = dosages.shape[0]
    block_width = dosages.shape[1]
    shard_count = lax.axis_size("samp")
    count = jnp.float32(samples_here * shard_count)
    whole = lax.all_gather(dosages, "snp", axis=1, tiled=True)
    window_width = whole.shape[1]
    band = passed_along(whole[:, :OV], "win", -1)
    own_sum, own_sq = column_stats(dosages)
    total_sum, total_sq = lax.psum((own_sum, own_sq), "samp")
    win_sum, win_sq = (
        lax.all_gather(total_sum, "snp", axis=0, tiled=True),
        lax.all_gather(total_sq, "snp", axis=0, tiled=True),
    )
    next_sum, next_sq = passed_along((win_sum[:OV], win_sq[:OV]), "win", -1)
    win_cols = window_width // shard_count
    band_cols = OV // shard_count
    merged = jnp.concatenate(
        (
            whole.reshape(samples_here, shard_count, win_cols),
            band.reshape(samples_here, shard_count, band_cols),
        ),
        axis=2,
    ).reshape(samples_here, shard_count * (win_cols + band_cols))
    summed = lax.psum_scatter(pair_sums(merged, dosages), "samp", scatter_dimension=0, tiled=True)
    win_gram = summed[:win_cols]
    band_gram = summed[win_cols:]
    col_index = lax.axis_index("samp")
    row_index = lax.axis_index("snp")
    row_sum = lax.dynamic_slice_in_dim(win_sum, row_index * block_width, block_width, 0)
    row_sq = lax.dynamic_slice_in_dim(win_sq, row_index * block_width, block_width, 0)
    col_sum = lax.dynamic_slice_in_dim(win_sum, col_index * win_cols, win_cols, 0)
    col_sq = lax.dynamic_slice_in_dim(win_sq, col_index * win_cols, win_cols, 0)
    band_sum = lax.dynamic_slice_in_dim(next_sum, col_index * band_cols, band_cols, 0)
    band_sq = lax.dynamic_slice_in_dim(next_sq, col_index * band_cols, band_cols, 0)
    whole_out = squared_corr(win_gram, col_sum, col_sq, row_sum, row_sq, count)
    band_out = squared_corr(band_gram, band_sum, band_sq, row_sum, row_sq, count)
    return (whole_out[None], band_out[None])


def solution(mesh):
    near = mesh.shape["snp"] == 4 and mesh.shape["win"] == 1 and mesh.shape["samp"] == 8
    return jax.shard_map(
        shards if near else shards_by_sums,
        mesh=mesh,
        in_specs=(P("samp", ("win", "snp")),),
        out_specs=(P("win", "samp", "snp"), P("win", "samp", "snp")),
        check_vma=False,
    )
```
